128 devices in a mesh: row: 16 (over y, x_lo, core), col: 8 (over x_hi, z).
Axes of the slice: x: 4 (x_hi: 2, x_lo: 2; x = x_hi * 2 + x_lo), y: 4, z: 4, core: 2. Of those that a mesh axis runs over, the one named last changes fastest.
Arguments:
- adjacency: int32 [10240, 320], P('row', 'col'), may hold values from -2147483648 to 2147483647, as said below
- relabel: int32 [10240], P(('row', 'col')), may hold values from 0 to 10239, each once
Outputs:
- clustering: float32 [10240], P(('row', 'col'))
- transitivity: float32 [], replicated
The draws below stay inside these ranges and needn't reach their ends.
Inputs may be any that keep to these rules, and one draw needn't show every extreme that they name: The unpacked adjacency is symmetric with a zero diagonal.
All inputs are finite; a program needn't handle non-finite values.
Results may differ from the reference program's by a relative error of at most 0.0003.
Values sent between devices are 32-bit elements.
No kernel may reach another device: no remote copies, remote signals or barrier semaphores. Data moves between devices by JAX's collectives and lax.ppermute only.
A program may use at most 128 MiB of HBM per device.

```python
import jax
import jax.numpy as jnp
from jax import lax

NV = 10240
N_ROW = 16


def draw_adjacency(key, part):
    first, second = jax.random.split(jax.random.fold_in(key, 23), 2)
    activity = jax.random.randint(first, (NV,), 1, 5)
    thresh = 1000 * activity[:, None] * activity[None, :]
    coins = jax.random.randint(second, (NV, NV), 0, 65536)
    keep = coins < thresh
    index = jnp.arange(NV)
    upper = keep & (index[None, :] > index[:, None])
    links = (upper | upper.T).astype(jnp.int32)
    bits = links.reshape(NV, NV // 32, 32)
    shifts = jnp.arange(32, dtype=jnp.int32)
    words = jnp.sum(lax.shift_left(bits, shifts[None, None, :]), axis=2)
    return words.astype(jnp.int32)


def setup_inputs(seed: int = 0) -> dict:
    key_list = jax.random.split(jax.random.key(seed), 3)
    return {
        "adjacency": draw_adjacency(jax.random.fold_in(key_list[2], 71), 0),
        "relabel": jax.random.permutation(key_list[1], NV).astype(jnp.int32),
    }


def unpack(words):
    shifts = jnp.arange(32, dtype=jnp.int32)
    bits = lax.shift_right_logical(words[:, :, None], shifts[None, None, :]) & 1
    return bits.reshape(words.shape[0], words.shape[1] * 32).astype(jnp.bfloat16)


def reference(adjacency, relabel):
    links = unpack(adjacency)
    block_rows = NV // N_ROW
    starts = jnp.arange(N_ROW, dtype=jnp.int32) * block_rows

    def one_block(offset):
        rows = lax.dynamic_slice_in_dim(links, offset.astype(jnp.int32), block_rows, 0)
        paths = jnp.dot(rows, links, preferred_element_type=jnp.float32)
        wide = rows.astype(jnp.float32)
        return jnp.sum(wide * paths, axis=1), jnp.sum(wide, axis=1)

    closed, degree = lax.map(one_block, starts)
    closed = closed.reshape(NV)
    degree = degree.reshape(NV)
    wedges = jnp.maximum(degree * (degree - 1.0), 1.0)
    ratio = closed / wedges
    clustering = jnp.take(ratio, relabel, axis=0)
    transitivity = jnp.sum(closed) / jnp.sum(wedges)
    return clustering, transitivity
```

```python
import jax
import jax.numpy as jnp
from jax import lax
from jax.experimental import pallas as pl
from jax.experimental.pallas import tpu as pltpu
from jax.sharding import PartitionSpec as P

ALL = ("row", "col")
WINDOW = 5
WEIGHTS = (1.0, 2.0, 2.0, 2.0, 1.0)


def spread(value, peers):
    return jnp.broadcast_to(value[None], (peers, *value.shape))


def unpacked(row, value, dtype):
    lanes = row.shape[1]
    bit = lax.broadcasted_iota(jnp.int32, (32, lanes), 0)
    hit = (row & lax.shift_left(jnp.int32(1), bit)) != 0
    return jnp.where(hit, jnp.float32(value), jnp.float32(0)).astype(dtype)


def count_kernel(own, oth, r0, r1, r2, r3, r4, out, rhs, lhs, acc, *, dtype):
    core = lax.rem(lax.axis_index("row"), 2)
    col = lax.axis_index("col")
    words, lanes = r0.shape
    half = words // 2
    depth = words * 32
    rows = (r0, r1, r2, r3, r4)
    for t in range(WINDOW):

        def fill_rhs(w, _, t=t):
            src = lax.rem(core * half + w, words)
            at = pl.multiple_of(t * depth + w * 32, 32)
            rhs[pl.ds(at, 32), :] = unpacked(rows[t][pl.ds(src, 1), :], WEIGHTS[t], dtype)
            return 0

        lax.fori_loop(0, words, fill_rhs, 0)

    acc[...] = jnp.zeros_like(acc)

    def step(t, _):
        block = lax.rem(col + t, 8)

        def fill_lhs(w, _):
            at = pl.multiple_of(w * 32, 32)
            lhs[pl.ds(at, 32), :lanes] = unpacked(own[block, pl.ds(w, 1), :], 1.0, dtype)
            lhs[pl.ds(at, 32), lanes:] = unpacked(oth[block, pl.ds(w, 1), :], 1.0, dtype)
            return 0

        lax.fori_loop(0, words, fill_lhs, 0)
        at = pl.multiple_of(t * depth, depth)
        acc[...] += jnp.dot(
            lhs[...], rhs[pl.ds(at, depth), :], preferred_element_type=jnp.float32
        )
        return 0

    lax.fori_loop(0, WINDOW, step, 0)

    def masked(w, total):
        at = pl.multiple_of(w * 32, 32)
        bit = lax.broadcasted_iota(jnp.int32, (32, lanes), 0)
        hit = (r0[pl.ds(w, 1), :] & lax.shift_left(jnp.int32(1), bit)) != 0
        picked = jnp.where(hit, acc[pl.ds(at, 32), :], 0.0)
        return total + picked.reshape(4, 8, lanes).sum(axis=0)

    total = lax.fori_loop(0, words, masked, jnp.zeros((8, lanes), jnp.float32))
    closed = jnp.sum(total, axis=0, keepdims=True)
    links = sum(lax.population_count(rows[t][...]) for t in range(4))
    degree = jnp.sum(links, axis=0, keepdims=True).astype(jnp.float32)
    degree = jnp.concatenate([degree, jnp.zeros((1, 128), jnp.float32)], axis=1)
    part = lax.rem(col, 4)
    window = jnp.where(
        part == 0, degree[:, :256], jnp.where(part == 1, degree[:, 256:512], degree[:, 512:768])
    )
    payload = jnp.concatenate([closed, window], axis=1)
    out[...] = jnp.broadcast_to(payload, out.shape)


def finish_kernel(parts, relabel, clustering, transitivity):
    value = parts[...].reshape(16, 8, 896)
    closed = value[:, :, :640].sum(axis=1)
    slot = lax.rem(lax.broadcasted_iota(jnp.int32, (16, 8, 256), 1), 4)
    window = value[:, :, 640:]
    pieces = [jnp.where(slot == m, window, 0.0).sum(axis=1) for m in range(3)]
    degree = jnp.concatenate([pieces[0], pieces[1], pieces[2][:, :128]], axis=1)
    wedges = jnp.maximum(degree * (degree - 1.0), 1.0)
    ratio = closed / wedges
    index = relabel[...]
    block = index // 640
    lane = index - block * 640
    hot = (lax.broadcasted_iota(jnp.int32, (640, 80), 0) == lane).astype(jnp.float32)
    picked = jnp.dot(
        ratio, hot, preferred_element_type=jnp.float32, precision=lax.Precision.HIGHEST
    )
    mine = lax.broadcasted_iota(jnp.int32, (16, 80), 0) == block
    clustering[...] = jnp.sum(jnp.where(mine, picked, 0.0), axis=0, keepdims=True)
    total = jnp.sum(jnp.sum(closed, axis=0, keepdims=True), axis=1, keepdims=True)
    pairs = jnp.sum(jnp.sum(wedges, axis=0, keepdims=True), axis=1, keepdims=True)
    transitivity[...] = total / pairs


def body(adjacency, relabel, dtype=jnp.bfloat16):
    words = adjacency.T
    rows = [words] + [
        lax.ppermute(words, "col", [((c + t) % 8, c) for c in range(8)])
        for t in range(1, WINDOW)
    ]
    cores = [[2 * chip + core for chip in range(8)] for core in range(2)]
    own = lax.all_to_all(
        spread(words, 8), "row", 0, 0, axis_index_groups=cores, tiled=True
    )
    oth = lax.ppermute(own, "row", [(r, r ^ 1) for r in range(16)])
    vmem = pl.BlockSpec(memory_space=pltpu.VMEM)
    depth = words.shape[0] * 32
    lanes = words.shape[1]

    def kernel(*refs):
        count_kernel(*refs, dtype=dtype)

    payload = pl.pallas_call(
        kernel,
        out_shape=jax.ShapeDtypeStruct((128, 896), jnp.float32),
        in_specs=[vmem] * 7,
        out_specs=vmem,
        scratch_shapes=[
            pltpu.VMEM((WINDOW * depth, lanes), dtype),
            pltpu.VMEM((depth, depth), dtype),
            pltpu.VMEM((depth, lanes), jnp.float32),
        ],
        compiler_params=pltpu.CompilerParams(vmem_limit_bytes=60 * 2**20),
        name="count",
    )(own, oth, *rows)
    parts = lax.all_to_all(payload, ALL, 0, 0, tiled=True)
    clustering, transitivity = pl.pallas_call(
        finish_kernel,
        out_shape=(
            jax.ShapeDtypeStruct((1, 80), jnp.float32),
            jax.ShapeDtypeStruct((1, 1), jnp.float32),
        ),
        in_specs=[vmem] * 2,
        out_specs=(vmem, vmem),
        name="finish",
    )(parts, relabel[None])
    return clustering[0], transitivity[0, 0]


def solution(mesh):
    return jax.shard_map(
        body,
        mesh=mesh,
        in_specs=(P("row", "col"), P(ALL)),
        out_specs=(P(ALL), P()),
        check_vma=False,
    )
```

```python
import jax
import jax.numpy as jnp
from jax import lax
from jax.experimental import pallas as pl
from jax.experimental.pallas import tpu as pltpu
from jax.sharding import PartitionSpec as P

ALL = ("row", "col")
WINDOW = 5


def spread(value, peers):
    return jnp.broadcast_to(value[None], (peers, *value.shape))


def shifted(row, step):
    words = jnp.broadcast_to(row, (32, row.shape[1]))
    return lax.shift_right_logical(words, step)


def zero_one(row, dtype):
    bit = lax.broadcasted_iota(jnp.int32, (32, row.shape[1]), 0)
    value = (shifted(row, bit) & 1).astype(jnp.int8)
    return value.astype(jnp.bfloat16).astype(dtype)


def scaled_bits(row, dtype):
    bit = lax.broadcasted_iota(jnp.int32, (32, row.shape[1]), 0)
    octet = shifted(row, (bit // 8) * 8).astype(jnp.int8)
    mask = lax.shift_left(jnp.int32(1), bit % 8).astype(jnp.int8)
    return (octet & mask).astype(jnp.bfloat16).astype(dtype)


ORDER = (0, 4, 1, 2, 3)


def expand_kernel(r0, r1, r2, r3, r4, rhs, window, *, dtype):
    core = lax.rem(lax.axis_index("row"), 2)
    part = lax.rem(lax.axis_index("col"), 4)
    words = r0.shape[0]
    half = words // 2
    depth = words * 32
    rows = (r0, r1, r2, r3, r4)
    for k, t in enumerate(ORDER):

        def fill_rhs(w, _, k=k, t=t):
            src = lax.rem(core * half + w, words)
            at = pl.multiple_of(k * depth + w * 32, 32)
            rhs[pl.ds(at, 32), :] = zero_one(rows[t][pl.ds(src, 1), :], dtype)
            return 0

        lax.fori_loop(0, words, fill_rhs, 0, unroll=4)
    links = sum(lax.population_count(rows[t][...]) for t in range(4))
    degree = jnp.sum(links, axis=0, keepdims=True).astype(jnp.float32)
    first = jnp.where(
        part == 0,
        degree[:, :128],
        jnp.where(part == 1, degree[:, 256:384], degree[:, 512:]),
    )
    second = jnp.where(part == 0, degree[:, 128:256], degree[:, 384:512])
    window[...] = jnp.concatenate([first, second], axis=0)


def count_kernel(own, oth, r0, rhs, window, out, left, right, *, dtype, group):
    col = lax.axis_index("col")
    words, lanes = r0.shape
    depth = words * 32
    blocks = [lax.rem(col + t, 8) for t in ORDER]
    once = 2 * depth

    def fill(tile, start):
        for w in range(group):
            for k, block in enumerate(blocks):
                for side, source in enumerate((own, oth)):
                    at = k * depth + side * lanes
                    tile[w * 32 : w * 32 + 32, at : at + lanes] = scaled_bits(
                        source[block, pl.ds(start + w, 1), :], dtype
                    )

    bit = lax.broadcasted_iota(jnp.int32, (32, lanes), 0)
    spot = lax.shift_left(jnp.int32(1), bit)
    octave = lax.shift_left(jnp.int32(1), bit % 8).astype(jnp.float32)
    undo = jnp.where(bit % 8 == 7, -1.0, 1.0) / octave

    def use(tile, start, total):
        paths = jnp.dot(
            tile[:, :once], rhs[:once, :], preferred_element_type=jnp.float32
        ) + 2.0 * jnp.dot(
            tile[:, once:], rhs[once:, :], preferred_element_type=jnp.float32
        )
        for w in range(group):
            hit = (r0[pl.ds(start + w, 1), :] & spot) != 0
            picked = jnp.where(hit, paths[w * 32 : w * 32 + 32] * undo, 0.0)
            total = total + picked.reshape(4, 8, lanes).sum(axis=0)
        return total

    fill(left, 0)

    def pair(step, total):
        start = step * 2 * group
        fill(right, start + group)
        total = use(left, start, total)
        fill(left, lax.rem(start + 2 * group, words))
        return use(right, start + group, total)

    total = lax.fori_loop(
        0, words // (2 * group), pair, jnp.zeros((8, lanes), jnp.float32)
    )
    closed = jnp.sum(total, axis=0, keepdims=True)
    payload = jnp.concatenate(
        [closed[:, 128 * j : 128 * j + 128] for j in range(5)]
        + [window[...], window[:1, :]],
        axis=0,
    )
    out[...] = jnp.broadcast_to(payload[None], out.shape)


def finish_kernel(parts, relabel, clustering, transitivity):
    value = parts[...].reshape(16, 8, 8, 128)
    closed = value[:, :, :5].sum(axis=1)
    slots = [value[:, m, 5:7] + value[:, m + 4, 5:7] for m in range(3)]
    degree = jnp.concatenate([slots[0], slots[1], slots[2][:, :1]], axis=1)
    wedges = jnp.maximum(degree * (degree - 1.0), 1.0)
    ratio = (closed / wedges).reshape(80, 128)
    index = relabel[...]
    line = index // 128
    lane = index - line * 128
    hot = (lax.broadcasted_iota(jnp.int32, (128, 80), 0) == lane).astype(jnp.float32)
    picked = jnp.dot(
        ratio, hot, preferred_element_type=jnp.float32, precision=lax.Precision.HIGHEST
    )
    mine = lax.broadcasted_iota(jnp.int32, (80, 80), 0) == line
    clustering[...] = jnp.sum(jnp.where(mine, picked, 0.0), axis=0, keepdims=True)
    total = jnp.sum(closed.reshape(80, 128), axis=0, keepdims=True)
    pairs = jnp.sum(wedges.reshape(80, 128), axis=0, keepdims=True)
    transitivity[...] = jnp.sum(total, axis=1, keepdims=True) / jnp.sum(
        pairs, axis=1, keepdims=True
    )


def body(adjacency, relabel, dtype=jnp.float8_e4m3fn, group=10):
    words = adjacency.T
    cores = [[2 * chip + core for chip in range(8)] for core in range(2)]
    own = lax.all_to_all(
        spread(words, 8), "row", 0, 0, axis_index_groups=cores, tiled=True
    )
    rows = [words]
    for t in range(1, WINDOW):
        rows.append(lax.ppermute(words, "col", [((c + t) % 8, c) for c in range(8)]))
    oth = lax.ppermute(own, "row", [(r, r ^ 1) for r in range(16)])
    vmem = pl.BlockSpec(memory_space=pltpu.VMEM)
    depth = words.shape[0] * 32
    lanes = words.shape[1]

    def expand(*refs):
        expand_kernel(*refs, dtype=dtype)

    def count(*refs):
        count_kernel(*refs, dtype=dtype, group=group)

    rhs, window = pl.pallas_call(
        expand,
        out_shape=(
            jax.ShapeDtypeStruct((WINDOW * depth, lanes), dtype),
            jax.ShapeDtypeStruct((2, 128), jnp.float32),
        ),
        in_specs=[vmem] * WINDOW,
        out_specs=(vmem, vmem),
        compiler_params=pltpu.CompilerParams(vmem_limit_bytes=12 * 2**20),
        cost_estimate=pl.CostEstimate(
            flops=10**9, bytes_accessed=5 * 10**6, transcendentals=0
        ),
        name="expand",
    )(*rows)
    payload = pl.pallas_call(
        count,
        out_shape=jax.ShapeDtypeStruct((128, 8, 128), jnp.float32),
        in_specs=[vmem] * 5,
        out_specs=vmem,
        scratch_shapes=[
            pltpu.VMEM((group * 32, WINDOW * depth), dtype),
            pltpu.VMEM((group * 32, WINDOW * depth), dtype),
        ],
        compiler_params=pltpu.CompilerParams(vmem_limit_bytes=30 * 2**20),
        name="count",
    )(own, oth, words, rhs, window)
    parts = lax.all_to_all(payload, ALL, 0, 0, tiled=True)
    clustering, transitivity = pl.pallas_call(
        finish_kernel,
        out_shape=(
            jax.ShapeDtypeStruct((1, 80), jnp.float32),
            jax.ShapeDtypeStruct((1, 1), jnp.float32),
        ),
        in_specs=[vmem] * 2,
        out_specs=(vmem, vmem),
        name="finish",
    )(parts, relabel[None])
    return clustering[0], transitivity[0, 0]


def solution(mesh):
    return jax.shard_map(
        body,
        mesh=mesh,
        in_specs=(P("row", "col"), P(ALL)),
        out_specs=(P(ALL), P()),
        check_vma=False,
    )
```

```python
import jax
import jax.numpy as jnp
from jax import lax
from jax.experimental import pallas as pl
from jax.experimental.pallas import tpu as pltpu
from jax.sharding import PartitionSpec as P

ALL = ("row", "col")
WINDOW = 5


def spread(value, peers):
    return jnp.broadcast_to(value[None], (peers, *value.shape))


def shifted(row, step):
    words = jnp.broadcast_to(row, (32, row.shape[1]))
    return lax.shift_right_logical(words, step)


def zero_one(row, dtype):
    bit = lax.broadcasted_iota(jnp.int32, (32, row.shape[1]), 0)
    value = (shifted(row, bit) & 1).astype(jnp.int8)
    return value.astype(jnp.bfloat16).astype(dtype)


def scaled_bits(row, dtype):
    bit = lax.broadcasted_iota(jnp.int32, (32, row.shape[1]), 0)
    octet = shifted(row, (bit // 8) * 8).astype(jnp.int8)
    mask = lax.shift_left(jnp.int32(1), bit % 8).astype(jnp.int8)
    return (octet & mask).astype(jnp.bfloat16).astype(dtype)


ORDER = (0, 1, 4, 2, 3)
EARLY = ORDER[:2]
LATE = ORDER[2:]


def expand_kernel(*refs, dtype):
    core = lax.rem(lax.axis_index("row"), 2)
    rows, rhs, tally = refs[:-2], refs[-2], refs[-1]
    words = rows[0].shape[0]
    half = words // 2
    depth = words * 32
    for k, row in enumerate(rows):

        def fill_rhs(w, _, k=k, row=row):
            src = lax.rem(core * half + w, words)
            at = pl.multiple_of(k * depth + w * 32, 32)
            rhs[pl.ds(at, 32), :] = zero_one(row[pl.ds(src, 1), :], dtype)
            return 0

        lax.fori_loop(0, words, fill_rhs, 0, unroll=4)
    links = sum(lax.population_count(row[...]) for row in rows[-2:])
    tally[...] = jnp.sum(links, axis=0, keepdims=True).astype(jnp.float32)


def count_kernel(own, oth, r0, early, late, near, far, out, left, right, *, dtype, group):
    col = lax.axis_index("col")
    words, lanes = r0.shape
    depth = words * 32
    blocks = [lax.rem(col + t, 8) for t in ORDER]

    def fill(tile, start):
        for w in range(group):
            for k, block in enumerate(blocks):
                for side, source in enumerate((own, oth)):
                    at = k * depth + side * lanes
                    tile[w * 32 : w * 32 + 32, at : at + lanes] = scaled_bits(
                        source[block, pl.ds(start + w, 1), :], dtype
                    )

    bit = lax.broadcasted_iota(jnp.int32, (32, lanes), 0)
    spot = lax.shift_left(jnp.int32(1), bit)
    octave = lax.shift_left(jnp.int32(1), bit % 8).astype(jnp.float32)
    undo = jnp.where(bit % 8 == 7, -1.0, 1.0) / octave

    def use(tile, start, total):
        def times(first, rhs):
            count = rhs.shape[0]
            return jnp.dot(
                tile[:, first : first + count], rhs, preferred_element_type=jnp.float32
            )

        doubled = times(depth, early[depth:, :]) + times(3 * depth, late[depth:, :])
        paths = times(0, early[:depth, :]) + times(2 * depth, late[:depth, :])
        paths = paths + 2.0 * doubled
        for w in range(group):
            hit = (r0[pl.ds(start + w, 1), :] & spot) != 0
            picked = jnp.where(hit, paths[w * 32 : w * 32 + 32] * undo, 0.0)
            total = total + picked.reshape(4, 8, lanes).sum(axis=0)
        return total

    fill(left, 0)

    def pair(step, total):
        start = step * 2 * group
        fill(right, start + group)
        total = use(left, start, total)
        fill(left, lax.rem(start + 2 * group, words))
        return use(right, start + group, total)

    total = lax.fori_loop(
        0, words // (2 * group), pair, jnp.zeros((8, lanes), jnp.float32)
    )
    closed = jnp.sum(total, axis=0, keepdims=True)
    degree = near[...] + far[...]
    part = lax.rem(col, 4)
    first = jnp.where(
        part == 0,
        degree[:, :128],
        jnp.where(part == 1, degree[:, 256:384], degree[:, 512:]),
    )
    second = jnp.where(part == 0, degree[:, 128:256], degree[:, 384:512])
    payload = jnp.concatenate(
        [closed[:, 128 * j : 128 * j + 128] for j in range(5)] + [first, second, first],
        axis=0,
    )
    out[...] = jnp.broadcast_to(payload[None], out.shape)


def finish_kernel(parts, relabel, clustering, transitivity):
    value = parts[...].reshape(16, 8, 8, 128)
    closed = value[:, :, :5].sum(axis=1)
    slots = [value[:, m, 5:7] + value[:, m + 4, 5:7] for m in range(3)]
    degree = jnp.concatenate([slots[0], slots[1], slots[2][:, :1]], axis=1)
    wedges = jnp.maximum(degree * (degree - 1.0), 1.0)
    ratio = (closed / wedges).reshape(80, 128)
    index = relabel[...]
    line = index // 128
    lane = index - line * 128
    hot = (lax.broadcasted_iota(jnp.int32, (128, 80), 0) == lane).astype(jnp.float32)
    picked = jnp.dot(
        ratio, hot, preferred_element_type=jnp.float32, precision=lax.Precision.HIGHEST
    )
    mine = lax.broadcasted_iota(jnp.int32, (80, 80), 0) == line
    clustering[...] = jnp.sum(jnp.where(mine, picked, 0.0), axis=0, keepdims=True)
    total = jnp.sum(closed.reshape(80, 128), axis=0, keepdims=True)
    pairs = jnp.sum(wedges.reshape(80, 128), axis=0, keepdims=True)
    transitivity[...] = jnp.sum(total, axis=1, keepdims=True) / jnp.sum(
        pairs, axis=1, keepdims=True
    )


def body(adjacency, relabel, dtype=jnp.float8_e4m3fn, group=10):
    words = adjacency.T
    cores = [[2 * chip + core for chip in range(8)] for core in range(2)]
    own = lax.all_to_all(
        spread(words, 8), "row", 0, 0, axis_index_groups=cores, tiled=True
    )
    rows = [words]
    for t in range(1, WINDOW):
        rows.append(lax.ppermute(words, "col", [((c + t) % 8, c) for c in range(8)]))
    oth = lax.ppermute(own, "row", [(r, r ^ 1) for r in range(16)])
    vmem = pl.BlockSpec(memory_space=pltpu.VMEM)
    depth = words.shape[0] * 32
    lanes = words.shape[1]

    def count(*refs):
        count_kernel(*refs, dtype=dtype, group=group)

    def expand(picks):
        def kernel(*refs):
            expand_kernel(*refs, dtype=dtype)

        return pl.pallas_call(
            kernel,
            out_shape=(
                jax.ShapeDtypeStruct((len(picks) * depth, lanes), dtype),
                jax.ShapeDtypeStruct((1, lanes), jnp.float32),
            ),
            in_specs=[vmem] * len(picks),
            out_specs=(vmem, vmem),
            compiler_params=pltpu.CompilerParams(vmem_limit_bytes=12 * 2**20),
            cost_estimate=pl.CostEstimate(
                flops=4 * 10**8, bytes_accessed=3 * 10**6, transcendentals=0
            ),
        )(*[rows[t] for t in picks])

    early, near = expand(EARLY)
    late, far = expand(LATE)
    payload = pl.pallas_call(
        count,
        out_shape=jax.ShapeDtypeStruct((128, 8, 128), jnp.float32),
        in_specs=[vmem] * 7,
        out_specs=vmem,
        scratch_shapes=[
            pltpu.VMEM((group * 32, WINDOW * depth), dtype),
            pltpu.VMEM((group * 32, WINDOW * depth), dtype),
        ],
        compiler_params=pltpu.CompilerParams(vmem_limit_bytes=30 * 2**20),
        name="count",
    )(own, oth, words, early, late, near, far)
    parts = lax.all_to_all(payload, ALL, 0, 0, tiled=True)
    clustering, transitivity = pl.pallas_call(
        finish_kernel,
        out_shape=(
            jax.ShapeDtypeStruct((1, 80), jnp.float32),
            jax.ShapeDtypeStruct((1, 1), jnp.float32),
        ),
        in_specs=[vmem] * 2,
        out_specs=(vmem, vmem),
        name="finish",
    )(parts, relabel[None])
    return clustering[0], transitivity[0, 0]


def solution(mesh):
    return jax.shard_map(
        body,
        mesh=mesh,
        in_specs=(P("row", "col"), P(ALL)),
        out_specs=(P(ALL), P()),
        check_vma=False,
    )
```

```python
import jax
import jax.numpy as jnp
from jax import lax
from jax.experimental import pallas as pl
from jax.experimental.pallas import tpu as pltpu
from jax.sharding import PartitionSpec as P

ALL = ("row", "col")
WINDOW = 5


def spread(value, peers):
    return jnp.broadcast_to(value[None], (peers, *value.shape))


def shifted(row, step):
    words = jnp.broadcast_to(row, (32, row.shape[1]))
    return lax.shift_right_logical(words, step)


def zero_one(row, dtype):
    bit = lax.broadcasted_iota(jnp.int32, (32, row.shape[1]), 0)
    value = (shifted(row, bit) & 1).astype(jnp.int8)
    return value.astype(jnp.bfloat16).astype(dtype)


def scaled_bits(row, dtype):
    bit = lax.broadcasted_iota(jnp.int32, (32, row.shape[1]), 0)
    octet = shifted(row, (bit // 8) * 8).astype(jnp.int8)
    mask = lax.shift_left(jnp.int32(1), bit % 8).astype(jnp.int8)
    return (octet & mask).astype(jnp.bfloat16).astype(dtype)


ORDER = (0, 1, 4, 2, 3)
EARLY = ORDER[:2]
LATE = ORDER[2:]


def expand_kernel(*refs, dtype):
    core = lax.rem(lax.axis_index("row"), 2)
    rows, rhs, tally = refs[:-2], refs[-2], refs[-1]
    words = rows[0].shape[0]
    half = words // 2
    depth = words * 32
    for k, row in enumerate(rows):

        def fill_rhs(w, _, k=k, row=row):
            src = lax.rem(core * half + w, words)
            at = pl.multiple_of(k * depth + w * 32, 32)
            rhs[pl.ds(at, 32), :] = zero_one(row[pl.ds(src, 1), :], dtype)
            return 0

        lax.fori_loop(0, words, fill_rhs, 0, unroll=4)
    links = sum(lax.population_count(row[...]) for row in rows[-2:])
    tally[...] = jnp.sum(links, axis=0, keepdims=True).astype(jnp.float32)


def count_kernel(*refs, picks, weights, group, finish):
    own, oth = refs[:2]
    rhs = refs[2]
    out, left, right = refs[-3:]
    col = lax.axis_index("col")
    blocks, words, lanes = own.shape
    depth = words * 32
    places = [lax.rem(col + t, blocks) for t in picks]
    if finish:
        mask, paths_in, near, far = refs[3:7]
        bit = lax.broadcasted_iota(jnp.int32, (32, lanes), 0)
        spot = lax.shift_left(jnp.int32(1), bit)
        octave = lax.shift_left(jnp.int32(1), bit % 8).astype(jnp.float32)
        undo = jnp.where(bit % 8 == 7, -1.0, 1.0) / octave

    def fill(tile, start):
        for w in range(group):
            for k, place in enumerate(places):
                for side, source in enumerate((own, oth)):
                    at = k * depth + side * lanes
                    tile[w * 32 : w * 32 + 32, at : at + lanes] = scaled_bits(
                        source[place, pl.ds(start + w, 1), :], tile.dtype
                    )

    def use(tile, start, total):
        paths = 0.0
        first = 0
        for weight in dict.fromkeys(weights):
            last = first + weights.count(weight) * depth
            paths = paths + weight * jnp.dot(
                tile[:, first:last], rhs[first:last, :], preferred_element_type=jnp.float32
            )
            first = last
        at = pl.multiple_of(start * 32, 32)
        if not finish:
            out[pl.ds(at, group * 32), :] = paths
            return total
        for w in range(group):
            hit = (mask[pl.ds(start + w, 1), :] & spot) != 0
            known = paths_in[pl.ds(pl.multiple_of(at + w * 32, 32), 32), :]
            value = (paths[w * 32 : w * 32 + 32] + known) * undo
            picked = jnp.where(hit, value, 0.0)
            total = total + picked.reshape(4, 8, lanes).sum(axis=0)
        return total

    fill(left, 0)

    def pair(step, total):
        start = step * 2 * group
        fill(right, start + group)
        total = use(left, start, total)
        fill(left, lax.rem(start + 2 * group, words))
        return use(right, start + group, total)

    total = lax.fori_loop(
        0, words // (2 * group), pair, jnp.zeros((8, lanes), jnp.float32)
    )
    if not finish:
        return
    closed = jnp.sum(total, axis=0, keepdims=True)
    degree = near[...] + far[...]
    part = lax.rem(col, 4)
    first = jnp.where(
        part == 0,
        degree[:, :128],
        jnp.where(part == 1, degree[:, 256:384], degree[:, 512:]),
    )
    second = jnp.where(part == 0, degree[:, 128:256], degree[:, 384:512])
    payload = jnp.concatenate(
        [closed[:, 128 * j : 128 * j + 128] for j in range(5)] + [first, second, first],
        axis=0,
    )
    out[...] = jnp.broadcast_to(payload[None], out.shape)


def finish_kernel(parts, relabel, clustering, transitivity):
    value = parts[...].reshape(16, 8, 8, 128)
    closed = value[:, :, :5].sum(axis=1)
    slots = [value[:, m, 5:7] + value[:, m + 4, 5:7] for m in range(3)]
    degree = jnp.concatenate([slots[0], slots[1], slots[2][:, :1]], axis=1)
    wedges = jnp.maximum(degree * (degree - 1.0), 1.0)
    ratio = (closed / wedges).reshape(80, 128)
    index = relabel[...]
    line = index // 128
    lane = index - line * 128
    hot = (lax.broadcasted_iota(jnp.int32, (128, 80), 0) == lane).astype(jnp.float32)
    picked = jnp.dot(
        ratio, hot, preferred_element_type=jnp.float32, precision=lax.Precision.HIGHEST
    )
    mine = lax.broadcasted_iota(jnp.int32, (80, 80), 0) == line
    clustering[...] = jnp.sum(jnp.where(mine, picked, 0.0), axis=0, keepdims=True)
    total = jnp.sum(closed.reshape(80, 128), axis=0, keepdims=True)
    pairs = jnp.sum(wedges.reshape(80, 128), axis=0, keepdims=True)
    transitivity[...] = jnp.sum(total, axis=1, keepdims=True) / jnp.sum(
        pairs, axis=1, keepdims=True
    )


def body(adjacency, relabel, dtype=jnp.float8_e4m3fn, group=10):
    words = adjacency.T
    cores = [[2 * chip + core for chip in range(8)] for core in range(2)]
    own = lax.all_to_all(
        spread(words, 8), "row", 0, 0, axis_index_groups=cores, tiled=True
    )
    rows = [words]
    for t in range(1, WINDOW):
        rows.append(lax.ppermute(words, "col", [((c + t) % 8, c) for c in range(8)]))
    oth = lax.ppermute(own, "row", [(r, r ^ 1) for r in range(16)])
    vmem = pl.BlockSpec(memory_space=pltpu.VMEM)
    depth = words.shape[0] * 32
    lanes = words.shape[1]

    def expand(picks):
        def kernel(*refs):
            expand_kernel(*refs, dtype=dtype)

        return pl.pallas_call(
            kernel,
            out_shape=(
                jax.ShapeDtypeStruct((len(picks) * depth, lanes), dtype),
                jax.ShapeDtypeStruct((1, lanes), jnp.float32),
            ),
            in_specs=[vmem] * len(picks),
            out_specs=(vmem, vmem),
            compiler_params=pltpu.CompilerParams(vmem_limit_bytes=12 * 2**20),
            cost_estimate=pl.CostEstimate(
                flops=4 * 10**8, bytes_accessed=3 * 10**6, transcendentals=0
            ),
        )(*[rows[t] for t in picks])

    early, near = expand(EARLY)
    late, far = expand(LATE)

    def count(picks, weights, operands, out_shape, finish):
        def kernel(*refs):
            count_kernel(*refs, picks=picks, weights=weights, group=group, finish=finish)

        tile = pltpu.VMEM((group * 32, len(picks) * depth), dtype)
        return pl.pallas_call(
            kernel,
            out_shape=jax.ShapeDtypeStruct(out_shape, jnp.float32),
            in_specs=[vmem] * len(operands),
            out_specs=vmem,
            scratch_shapes=[tile, tile],
            compiler_params=pltpu.CompilerParams(vmem_limit_bytes=24 * 2**20),
            cost_estimate=pl.CostEstimate(
                flops=2 * len(picks) * depth * depth * lanes,
                bytes_accessed=6 * 10**6,
                transcendentals=0,
            ),
        )(*operands)

    paths = count(EARLY, (1.0, 2.0), (own, oth, early), (depth, lanes), False)
    payload = count(
        LATE,
        (1.0, 2.0, 2.0),
        (own, oth, late, words, paths, near, far),
        (128, 8, 128),
        True,
    )
    parts = lax.all_to_all(payload, ALL, 0, 0, tiled=True)
    clustering, transitivity = pl.pallas_call(
        finish_kernel,
        out_shape=(
            jax.ShapeDtypeStruct((1, 80), jnp.float32),
            jax.ShapeDtypeStruct((1, 1), jnp.float32),
        ),
        in_specs=[vmem] * 2,
        out_specs=(vmem, vmem),
        compiler_params=pltpu.CompilerParams(vmem_limit_bytes=4 * 2**20),
        name="finish",
    )(parts, relabel[None])
    return clustering[0], transitivity[0, 0]


def solution(mesh):
    return jax.shard_map(
        body,
        mesh=mesh,
        in_specs=(P("row", "col"), P(ALL)),
        out_specs=(P(ALL), P()),
        check_vma=False,
    )
```

```python
import jax
import jax.numpy as jnp
from jax import lax
from jax.experimental import pallas as pl
from jax.experimental.pallas import tpu as pltpu
from jax.sharding import PartitionSpec as P

ALL = ("row", "col")
WINDOW = 5


def spread(value, peers):
    return jnp.broadcast_to(value[None], (peers, *value.shape))


def shifted(row, step):
    words = jnp.broadcast_to(row, (32, row.shape[1]))
    return lax.shift_right_logical(words, step)


def weighted(row, weight, dtype):
    bit = lax.broadcasted_iota(jnp.int32, (32, row.shape[1]), 0)
    value = (shifted(row, bit).astype(jnp.int8) & jnp.int8(1)).astype(jnp.bfloat16)
    return (value * weight if weight != 1 else value).astype(dtype)


FIRST = (((0, 0), (0, 2)),)
REST = (((1, 0), (1, 2)), ((0, 4), (1, 4)), ((0, 1), (1, 1)), ((0, 3), (1, 3)))
WEIGHTS = (1, 2, 2, 2, 1)


TILE = 256


def fill_right(target, rows, step, tile, core):
    half = 20
    for w in range(8 * tile, 8 * tile + 8):
        side, t = step[w // half]
        base = half * (core if side == 0 else 1 - core) + w % half
        target[w * 32 : w * 32 + 32, :] = weighted(
            rows[t][pl.ds(base, 1), :], WEIGHTS[t], target.dtype
        )


def fill_left(target, sources, step, tile, places):
    for k, (side, t) in enumerate(step):
        words = sources[side][places[t], 8 * tile : 8 * tile + 8, :]
        octets = jnp.concatenate(
            [lax.shift_right_logical(words, jnp.int32(8 * byte)) for byte in range(4)], axis=0
        ).astype(jnp.int8)
        for s in range(8):
            picked = octets & jnp.int8(-128 if s == 7 else 1 << s)
            at = tile * TILE + s * 32
            target[at : at + 32, k * 640 : k * 640 + 640] = picked.astype(
                jnp.bfloat16
            ).astype(target.dtype)


def label_of(col):
    return (col % 4) * 2 + col // 4


def place_of(label):
    return (label % 2) * 4 + (label % 8) // 2


def places_of(col):
    return [place_of(label_of(col) + t) for t in range(WINDOW)]


def early_kernel(r2, right):
    core = lax.rem(lax.axis_index("row"), 2)
    for w in range(20):
        right[w * 32 : w * 32 + 32, :] = weighted(
            r2[pl.ds(20 * core + w, 1), :], WEIGHTS[2], right.dtype
        )


def product(left, right, tile):
    return jnp.dot(
        left[tile * TILE : tile * TILE + TILE, :],
        right[...],
        preferred_element_type=jnp.float32,
    )


def begin_kernel(own, early, paths, left, right):
    chip = lax.axis_index("row") // 2
    core = lax.rem(lax.axis_index("row"), 2)
    places = places_of(lax.axis_index("col"))
    right[640:, :] = early[...]
    for w in range(20):
        right[w * 32 : w * 32 + 32, :] = weighted(
            own[chip, pl.ds(20 * core + w, 1), :], WEIGHTS[0], right.dtype
        )
    fill_left(left, (own,), FIRST[0], 0, places)
    for tile in range(5):
        if tile < 4:
            fill_left(left, (own,), FIRST[0], tile + 1, places)
        paths[tile * TILE : tile * TILE + TILE, :] = product(left, right, tile)


def count_kernel(own, oth, r1, r2, r3, r4, paths, out, la, lb, ra, rb, acc):
    chip = lax.axis_index("row") // 2
    core = lax.rem(lax.axis_index("row"), 2)
    col = lax.axis_index("col")
    places = places_of(col)
    mask = own.at[chip]
    rows = (mask, r1, r2, r3, r4)
    lanes = r1.shape[1]
    left, right = (la, lb), (ra, rb)
    for tile in range(5):
        fill_left(la, (own, oth), REST[0], tile, places)
        fill_right(ra, rows, REST[0], tile, core)
    total = jnp.zeros((8, lanes), jnp.float32)
    for k in range(len(REST)):
        now, later = k % 2, (k + 1) % 2
        known = paths if k == 0 else acc
        for tile in range(5):
            if k + 1 < len(REST):
                fill_left(left[later], (own, oth), REST[k + 1], tile, places)
                fill_right(right[later], rows, REST[k + 1], tile, core)
            piece = slice(tile * TILE, tile * TILE + TILE)
            value = known[piece, :] + product(left[now], right[now], tile)
            if k + 1 < len(REST):
                acc[piece, :] = value
                continue
            words = mask[8 * tile : 8 * tile + 8, :]
            for s in range(8):
                part = 0.0
                for byte in range(4):
                    at = s * 32 + byte * 8
                    spot = 8 * byte + s
                    hit = (words & jnp.int32(-(2**31) if spot == 31 else 1 << spot)) != 0
                    part = part + jnp.where(hit, value[at : at + 8, :], 0.0)
                total = total + part * (-(2.0**-7) if s == 7 else 2.0**-s)
    closed = jnp.sum(total, axis=0, keepdims=True)
    links = sum(lax.population_count(rows[t][...]) for t in range(4))
    degree = jnp.sum(links, axis=0, keepdims=True).astype(jnp.float32)
    part = label_of(col) % 4
    first = jnp.where(
        part == 0,
        degree[:, :128],
        jnp.where(part == 1, degree[:, 256:384], degree[:, 512:]),
    )
    second = jnp.where(part == 0, degree[:, 128:256], degree[:, 384:512])
    payload = jnp.concatenate(
        [closed[:, 128 * j : 128 * j + 128] for j in range(5)] + [first, second, first],
        axis=0,
    )
    out[...] = jnp.broadcast_to(payload[None], out.shape)


def finish_kernel(parts, relabel, clustering, transitivity):
    value = parts[...].reshape(16, 8, 8, 128)
    closed = value[:, :, :5].sum(axis=1)
    slots = [value[:, place_of(m), 5:7] + value[:, place_of(m + 4), 5:7] for m in range(3)]
    degree = jnp.concatenate([slots[0], slots[1], slots[2][:, :1]], axis=1)
    wedges = jnp.maximum(degree * (degree - 1.0), 1.0)
    ratio = (closed / wedges).reshape(80, 128)
    index = relabel[...]
    line = index // 128
    lane = index - line * 128
    hot = (lax.broadcasted_iota(jnp.int32, (128, 80), 0) == lane).astype(jnp.float32)
    picked = jnp.dot(
        ratio, hot, preferred_element_type=jnp.float32, precision=lax.Precision.HIGHEST
    )
    mine = lax.broadcasted_iota(jnp.int32, (80, 80), 0) == line
    clustering[...] = jnp.sum(jnp.where(mine, picked, 0.0), axis=0, keepdims=True)
    total = jnp.sum(closed.reshape(80, 128), axis=0, keepdims=True)
    pairs = jnp.sum(wedges.reshape(80, 128), axis=0, keepdims=True)
    transitivity[...] = jnp.sum(total, axis=1, keepdims=True) / jnp.sum(
        pairs, axis=1, keepdims=True
    )


def body(adjacency, relabel, dtype=jnp.float8_e4m3fn):
    words = adjacency.T
    cores = [[2 * chip + core for chip in range(8)] for core in range(2)]
    own = lax.all_to_all(
        spread(words, 8), "row", 0, 0, axis_index_groups=cores, tiled=True
    )
    rows = [words]
    for t in range(1, WINDOW):
        rows.append(
            lax.ppermute(
                words, "col", [(place_of(label_of(c) + t), c) for c in range(8)]
            )
        )
    oth = lax.ppermute(own, "row", [(r, r ^ 1) for r in range(16)])
    vmem = pl.BlockSpec(memory_space=pltpu.VMEM)
    depth = words.shape[0] * 32
    lanes = words.shape[1]
    left = pltpu.VMEM((depth, depth), dtype)
    right = pltpu.VMEM((depth, lanes), dtype)
    acc = pltpu.VMEM((depth, lanes), jnp.float32)

    def call(kernel, operands, out_shape, scratch, steps, mib):
        return pl.pallas_call(
            kernel,
            out_shape=out_shape,
            in_specs=[vmem] * len(operands),
            out_specs=vmem,
            scratch_shapes=scratch,
            compiler_params=pltpu.CompilerParams(vmem_limit_bytes=mib * 2**20),
            cost_estimate=pl.CostEstimate(
                flops=max(2 * steps * depth * depth * lanes, 10**8),
                bytes_accessed=5 * 10**6,
                transcendentals=0,
            ),
        )(*operands)

    early = call(
        early_kernel,
        rows[2:3],
        jax.ShapeDtypeStruct((depth // 2, lanes), dtype),
        [],
        0,
        4,
    )
    paths = call(
        begin_kernel,
        (own, early),
        jax.ShapeDtypeStruct((depth, lanes), jnp.float32),
        [left, right],
        len(FIRST),
        16,
    )
    payload = call(
        count_kernel,
        (own, oth, *rows[1:], paths),
        jax.ShapeDtypeStruct((128, 8, 128), jnp.float32),
        [left, left, right, right, acc],
        len(REST),
        24,
    )
    parts = lax.all_to_all(payload, ALL, 0, 0, tiled=True)
    clustering, transitivity = pl.pallas_call(
        finish_kernel,
        out_shape=(
            jax.ShapeDtypeStruct((1, 80), jnp.float32),
            jax.ShapeDtypeStruct((1, 1), jnp.float32),
        ),
        in_specs=[vmem] * 2,
        out_specs=(vmem, vmem),
        compiler_params=pltpu.CompilerParams(vmem_limit_bytes=4 * 2**20),
        name="finish",
    )(parts, relabel[None])
    return clustering[0], transitivity[0, 0]


def solution(mesh):
    return jax.shard_map(
        body,
        mesh=mesh,
        in_specs=(P("row", "col"), P(ALL)),
        out_specs=(P(ALL), P()),
        check_vma=False,
    )
```

```python
import jax
import jax.numpy as jnp
from jax import lax
from jax.experimental import pallas as pl
from jax.experimental.pallas import tpu as pltpu
from jax.sharding import PartitionSpec as P

ALL = ("row", "col")
WINDOW = 5


def spread(value, peers):
    return jnp.broadcast_to(value[None], (peers, *value.shape))


def shifted(row, step):
    words = jnp.broadcast_to(row, (32, row.shape[1]))
    return lax.shift_right_logical(words, step)


def weighted(row, weight, dtype):
    bit = lax.broadcasted_iota(jnp.int32, (32, row.shape[1]), 0)
    value = (shifted(row, bit).astype(jnp.int8) & jnp.int8(1)).astype(jnp.bfloat16)
    return (value * weight if weight != 1 else value).astype(dtype)


FIRST = (((0, 0), (0, 2)),)
REST = (((1, 0), (1, 2)), ((0, 4), (1, 4)), ((0, 1), (1, 1)), ((0, 3), (1, 3)))
WEIGHTS = (1, 2, 2, 2, 1)


TILE = 256


def fill_right(target, rows, step, tile, core):
    half = 20
    for w in range(8 * tile, 8 * tile + 8):
        side, t = step[w // half]
        base = half * (core if side == 0 else 1 - core) + w % half
        target[w * 32 : w * 32 + 32, :] = weighted(
            rows[t][pl.ds(base, 1), :], WEIGHTS[t], target.dtype
        )


def fill_left(target, sources, step, tile, places):
    for k, (side, t) in enumerate(step):
        words = sources[side][places[t], 8 * tile : 8 * tile + 8, :]
        octets = jnp.concatenate(
            [lax.shift_right_logical(words, jnp.int32(8 * byte)) for byte in range(4)], axis=0
        ).astype(jnp.int8)
        for s in range(8):
            picked = octets & jnp.int8(-128 if s == 7 else 1 << s)
            at = tile * TILE + s * 32
            target[at : at + 32, k * 640 : k * 640 + 640] = picked.astype(
                jnp.bfloat16
            ).astype(target.dtype)


def label_of(col):
    return (col % 4) * 2 + col // 4


def place_of(label):
    return (label % 2) * 4 + (label % 8) // 2


def places_of(col):
    return [place_of(label_of(col) + t) for t in range(WINDOW)]


def early_kernel(r0, r2, right_first, right_next):
    core = lax.rem(lax.axis_index("row"), 2)
    rows = (r0, None, r2)
    for tile in range(5):
        fill_right(right_first, rows, FIRST[0], tile, core)
        fill_right(right_next, rows, REST[0], tile, core)


def product(left, right, tile):
    return jnp.dot(
        left[tile * TILE : tile * TILE + TILE, :],
        right[...],
        preferred_element_type=jnp.float32,
    )


def begin_kernel(own, right, paths, left):
    places = places_of(lax.axis_index("col"))
    fill_left(left, (own,), FIRST[0], 0, places)
    for tile in range(5):
        if tile < 4:
            fill_left(left, (own,), FIRST[0], tile + 1, places)
        paths[tile * TILE : tile * TILE + TILE, :] = product(left, right, tile)


def count_kernel(own, oth, r1, r2, r3, r4, right_next, paths, out, la, lb, ra, rb, acc):
    chip = lax.axis_index("row") // 2
    core = lax.rem(lax.axis_index("row"), 2)
    col = lax.axis_index("col")
    places = places_of(col)
    mask = own.at[chip]
    rows = (mask, r1, r2, r3, r4)
    lanes = r1.shape[1]
    left, right = (la, lb), (ra, rb)
    for tile in range(5):
        fill_left(la, (own, oth), REST[0], tile, places)
    total = jnp.zeros((8, lanes), jnp.float32)
    for k in range(len(REST)):
        now, later = k % 2, (k + 1) % 2
        known = paths if k == 0 else acc
        for tile in range(5):
            if k + 1 < len(REST):
                fill_left(left[later], (own, oth), REST[k + 1], tile, places)
                fill_right(right[later], rows, REST[k + 1], tile, core)
            piece = slice(tile * TILE, tile * TILE + TILE)
            factor = right_next if k == 0 else right[now]
            value = known[piece, :] + product(left[now], factor, tile)
            if k + 1 < len(REST):
                acc[piece, :] = value
                continue
            words = mask[8 * tile : 8 * tile + 8, :]
            for s in range(8):
                part = 0.0
                for byte in range(4):
                    at = s * 32 + byte * 8
                    spot = 8 * byte + s
                    hit = (words & jnp.int32(-(2**31) if spot == 31 else 1 << spot)) != 0
                    part = part + jnp.where(hit, value[at : at + 8, :], 0.0)
                total = total + part * (-(2.0**-7) if s == 7 else 2.0**-s)
    closed = jnp.sum(total, axis=0, keepdims=True)
    links = sum(lax.population_count(rows[t][...]) for t in range(4))
    degree = jnp.sum(links, axis=0, keepdims=True).astype(jnp.float32)
    part = label_of(col) % 4
    first = jnp.where(
        part == 0,
        degree[:, :128],
        jnp.where(part == 1, degree[:, 256:384], degree[:, 512:]),
    )
    second = jnp.where(part == 0, degree[:, 128:256], degree[:, 384:512])
    payload = jnp.concatenate(
        [closed[:, 128 * j : 128 * j + 128] for j in range(5)] + [first, second, first],
        axis=0,
    )
    out[...] = jnp.broadcast_to(payload[None], out.shape)


def reduced(parts):
    value = parts[...].reshape(8, 8, 8, 128)
    closed = value[:, :, :5].sum(axis=1)
    slots = [value[:, place_of(m), 5:7] + value[:, place_of(m + 4), 5:7] for m in range(3)]
    return closed, jnp.concatenate([slots[0], slots[1], slots[2][:, :1]], axis=1)


def interleaved(mine, other, core):
    first = jnp.where(core == 0, mine, other)
    second = jnp.where(core == 0, other, mine)
    return jnp.stack([first, second], axis=1).reshape(16, 5, 128)


def finish_kernel(own, oth, relabel, clustering, transitivity):
    core = lax.rem(lax.axis_index("row"), 2)
    closed, degree = (
        interleaved(mine, other, core) for mine, other in zip(reduced(own), reduced(oth))
    )
    wedges = jnp.maximum(degree * (degree - 1.0), 1.0)
    ratio = (closed / wedges).reshape(80, 128)
    index = relabel[...]
    line = index // 128
    lane = index - line * 128
    hot = (lax.broadcasted_iota(jnp.int32, (128, 80), 0) == lane).astype(jnp.float32)
    picked = jnp.dot(
        ratio, hot, preferred_element_type=jnp.float32, precision=lax.Precision.HIGHEST
    )
    mine = lax.broadcasted_iota(jnp.int32, (80, 80), 0) == line
    clustering[...] = jnp.sum(jnp.where(mine, picked, 0.0), axis=0, keepdims=True)
    total = jnp.sum(closed.reshape(80, 128), axis=0, keepdims=True)
    pairs = jnp.sum(wedges.reshape(80, 128), axis=0, keepdims=True)
    transitivity[...] = jnp.sum(total, axis=1, keepdims=True) / jnp.sum(
        pairs, axis=1, keepdims=True
    )


def body(adjacency, relabel, dtype=jnp.float8_e4m3fn):
    words = adjacency.T
    cores = [[2 * chip + core for chip in range(8)] for core in range(2)]
    own = lax.all_to_all(
        spread(words, 8), "row", 0, 0, axis_index_groups=cores, tiled=True
    )
    rows = [words]
    for t in range(1, WINDOW):
        rows.append(
            lax.ppermute(
                words, "col", [(place_of(label_of(c) + t), c) for c in range(8)]
            )
        )
    oth = lax.ppermute(own, "row", [(r, r ^ 1) for r in range(16)])
    vmem = pl.BlockSpec(memory_space=pltpu.VMEM)
    depth = words.shape[0] * 32
    lanes = words.shape[1]
    left = pltpu.VMEM((depth, depth), dtype)
    right = pltpu.VMEM((depth, lanes), dtype)
    acc = pltpu.VMEM((depth, lanes), jnp.float32)

    def call(kernel, operands, out_shape, scratch, steps, mib):
        return pl.pallas_call(
            kernel,
            out_shape=out_shape,
            in_specs=[vmem] * len(operands),
            out_specs=jax.tree.map(lambda _: vmem, out_shape),
            scratch_shapes=scratch,
            compiler_params=pltpu.CompilerParams(vmem_limit_bytes=mib * 2**20),
            cost_estimate=pl.CostEstimate(
                flops=max(2 * steps * depth * depth * lanes, 10**8),
                bytes_accessed=5 * 10**6,
                transcendentals=0,
            ),
        )(*operands)

    operand = jax.ShapeDtypeStruct((depth, lanes), dtype)
    right_first, right_next = call(
        early_kernel, (rows[0], rows[2]), (operand, operand), [], 0, 8
    )
    paths = call(
        begin_kernel,
        (own, right_first),
        jax.ShapeDtypeStruct((depth, lanes), jnp.float32),
        [left],
        len(FIRST),
        16,
    )
    payload = call(
        count_kernel,
        (own, oth, *rows[1:], right_next, paths),
        jax.ShapeDtypeStruct((64, 8, 128), jnp.float32),
        [left, left, right, right, acc],
        len(REST),
        24,
    )
    peers = [
        [(2 * chip + core) * 8 + c for chip in range(8) for c in range(8)]
        for core in range(2)
    ]
    parts = lax.all_to_all(payload, ALL, 0, 0, axis_index_groups=peers, tiled=True)
    across = lax.ppermute(parts, "row", [(r, r ^ 1) for r in range(16)])
    clustering, transitivity = pl.pallas_call(
        finish_kernel,
        out_shape=(
            jax.ShapeDtypeStruct((1, 80), jnp.float32),
            jax.ShapeDtypeStruct((1, 1), jnp.float32),
        ),
        in_specs=[vmem] * 3,
        out_specs=(vmem, vmem),
        compiler_params=pltpu.CompilerParams(vmem_limit_bytes=4 * 2**20),
        name="finish",
    )(parts, across, relabel[None])
    return clustering[0], transitivity[0, 0]


def solution(mesh):
    return jax.shard_map(
        body,
        mesh=mesh,
        in_specs=(P("row", "col"), P(ALL)),
        out_specs=(P(ALL), P()),
        check_vma=False,
    )
```

```python
import jax
import jax.numpy as jnp
from jax import lax
from jax.experimental import pallas as pl
from jax.experimental.pallas import tpu as pltpu
from jax.sharding import PartitionSpec as P

ALL = ("row", "col")
WINDOW = 5


def spread(value, peers):
    return jnp.broadcast_to(value[None], (peers, *value.shape))


def shifted(row, step):
    words = jnp.broadcast_to(row, (32, row.shape[1]))
    return lax.shift_right_logical(words, step)


def weighted(row, weight, dtype):
    bit = lax.broadcasted_iota(jnp.int32, (32, row.shape[1]), 0)
    value = (shifted(row, bit).astype(jnp.int8) & jnp.int8(1)).astype(jnp.bfloat16)
    return (value * weight if weight != 1 else value).astype(dtype)


FIRST = (((0, 0), (0, 2)),)
REST = (((1, 0), (1, 2)), ((0, 4), (1, 4)), ((0, 1), (1, 1)), ((0, 3), (1, 3)))
WEIGHTS = (1, 2, 2, 2, 1)


TILE = 256


def fill_right(target, rows, step, tile, core):
    half = 20
    for w in range(8 * tile, 8 * tile + 8):
        side, t = step[w // half]
        base = half * (core if side == 0 else 1 - core) + w % half
        target[w * 32 : w * 32 + 32, :] = weighted(
            rows[t][pl.ds(base, 1), :], WEIGHTS[t], target.dtype
        )


def fill_left(target, sources, step, tile, places):
    for k, (side, t) in enumerate(step):
        words = sources[side][places[t], 8 * tile : 8 * tile + 8, :]
        octets = jnp.concatenate(
            [lax.shift_right_logical(words, jnp.int32(8 * byte)) for byte in range(4)], axis=0
        ).astype(jnp.int8)
        for s in range(8):
            picked = octets & jnp.int8(-128 if s == 7 else 1 << s)
            at = tile * TILE + s * 32
            target[at : at + 32, k * 640 : k * 640 + 640] = picked.astype(
                jnp.bfloat16
            ).astype(target.dtype)


def label_of(col):
    return (col % 4) * 2 + col // 4


def place_of(label):
    return (label % 2) * 4 + (label % 8) // 2


def places_of(col):
    return [place_of(label_of(col) + t) for t in range(WINDOW)]


def early_kernel(r0, r2, right_first, right_next):
    core = lax.rem(lax.axis_index("row"), 2)
    rows = (r0, None, r2)
    for tile in range(5):
        fill_right(right_first, rows, FIRST[0], tile, core)
        fill_right(right_next, rows, REST[0], tile, core)


def product(left, right, first, count):
    return jnp.dot(
        left[first : first + count, :], right[...], preferred_element_type=jnp.float32
    )


def begin_kernel(own, right, paths, left):
    places = places_of(lax.axis_index("col"))
    filled = 0
    for first in range(0, 1280, 640):
        while filled < 5 and filled * TILE < first + 2 * 640:
            fill_left(left, (own,), FIRST[0], filled, places)
            filled += 1
        paths[first : first + 640, :] = product(left, right, first, 640)


def count_kernel(own, oth, r1, r2, r3, r4, right_next, paths, out, la, lb, ra, rb, acc):
    chip = lax.axis_index("row") // 2
    core = lax.rem(lax.axis_index("row"), 2)
    col = lax.axis_index("col")
    places = places_of(col)
    mask = own.at[chip]
    rows = (mask, r1, r2, r3, r4)
    lanes = r1.shape[1]
    left, right = (la, lb), (ra, rb)
    for tile in range(5):
        fill_left(la, (own, oth), REST[0], tile, places)
    total = jnp.zeros((8, lanes), jnp.float32)
    size = 640
    for k in range(len(REST)):
        now, later = k % 2, (k + 1) % 2
        known = paths if k == 0 else acc
        factor = right_next if k == 0 else right[now]
        filled = 0
        for first in range(0, 1280, size):
            while k + 1 < len(REST) and filled < 5 and filled * TILE < first + size:
                fill_left(left[later], (own, oth), REST[k + 1], filled, places)
                fill_right(right[later], rows, REST[k + 1], filled, core)
                filled += 1
            value = known[first : first + size, :] + product(left[now], factor, first, size)
            if k + 1 < len(REST):
                acc[first : first + size, :] = value
                continue
            for chunk in range(first // 32, (first + size) // 32):
                tile, s = chunk // 8, chunk % 8
                words = mask[8 * tile : 8 * tile + 8, :]
                part = 0.0
                for byte in range(4):
                    at = chunk * 32 - first + byte * 8
                    spot = 8 * byte + s
                    hit = (words & jnp.int32(-(2**31) if spot == 31 else 1 << spot)) != 0
                    part = part + jnp.where(hit, value[at : at + 8, :], 0.0)
                total = total + part * (-(2.0**-7) if s == 7 else 2.0**-s)
    closed = jnp.sum(total, axis=0, keepdims=True)
    links = sum(lax.population_count(rows[t][...]) for t in range(4))
    degree = jnp.sum(links, axis=0, keepdims=True).astype(jnp.float32)
    part = label_of(col) % 4
    first = jnp.where(
        part == 0,
        degree[:, :128],
        jnp.where(part == 1, degree[:, 256:384], degree[:, 512:]),
    )
    second = jnp.where(part == 0, degree[:, 128:256], degree[:, 384:512])
    payload = jnp.concatenate(
        [closed[:, 128 * j : 128 * j + 128] for j in range(5)] + [first, second, first],
        axis=0,
    )
    out[...] = jnp.broadcast_to(payload[None], out.shape)


def reduced(parts):
    value = parts[...].reshape(8, 8, 8, 128)
    closed = value[:, :, :5].sum(axis=1)
    slots = [value[:, place_of(m), 5:7] + value[:, place_of(m + 4), 5:7] for m in range(3)]
    return closed, jnp.concatenate([slots[0], slots[1], slots[2][:, :1]], axis=1)


def interleaved(mine, other, core):
    first = jnp.where(core == 0, mine, other)
    second = jnp.where(core == 0, other, mine)
    return jnp.stack([first, second], axis=1).reshape(16, 5, 128)


def finish_kernel(own, oth, relabel, clustering, transitivity):
    core = lax.rem(lax.axis_index("row"), 2)
    closed, degree = (
        interleaved(mine, other, core) for mine, other in zip(reduced(own), reduced(oth))
    )
    wedges = jnp.maximum(degree * (degree - 1.0), 1.0)
    ratio = (closed / wedges).reshape(80, 128)
    index = relabel[...]
    line = index // 128
    lane = index - line * 128
    hot = (lax.broadcasted_iota(jnp.int32, (128, 80), 0) == lane).astype(jnp.float32)
    picked = jnp.dot(
        ratio, hot, preferred_element_type=jnp.float32, precision=lax.Precision.HIGHEST
    )
    mine = lax.broadcasted_iota(jnp.int32, (80, 80), 0) == line
    clustering[...] = jnp.sum(jnp.where(mine, picked, 0.0), axis=0, keepdims=True)
    total = jnp.sum(closed.reshape(80, 128), axis=0, keepdims=True)
    pairs = jnp.sum(wedges.reshape(80, 128), axis=0, keepdims=True)
    transitivity[...] = jnp.sum(total, axis=1, keepdims=True) / jnp.sum(
        pairs, axis=1, keepdims=True
    )


def body(adjacency, relabel, dtype=jnp.float8_e4m3fn):
    words = adjacency.T
    cores = [[2 * chip + core for chip in range(8)] for core in range(2)]
    own = lax.all_to_all(
        spread(words, 8), "row", 0, 0, axis_index_groups=cores, tiled=True
    )
    rows = [words]
    for t in range(1, WINDOW):
        rows.append(
            lax.ppermute(
                words, "col", [(place_of(label_of(c) + t), c) for c in range(8)]
            )
        )
    oth = lax.ppermute(own, "row", [(r, r ^ 1) for r in range(16)])
    vmem = pl.BlockSpec(memory_space=pltpu.VMEM)
    depth = words.shape[0] * 32
    lanes = words.shape[1]
    left = pltpu.VMEM((depth, depth), dtype)
    right = pltpu.VMEM((depth, lanes), dtype)
    acc = pltpu.VMEM((depth, lanes), jnp.float32)

    def call(kernel, operands, out_shape, scratch, steps, mib):
        return pl.pallas_call(
            kernel,
            out_shape=out_shape,
            in_specs=[vmem] * len(operands),
            out_specs=jax.tree.map(lambda _: vmem, out_shape),
            scratch_shapes=scratch,
            compiler_params=pltpu.CompilerParams(vmem_limit_bytes=mib * 2**20),
            cost_estimate=pl.CostEstimate(
                flops=max(2 * steps * depth * depth * lanes, 10**8),
                bytes_accessed=5 * 10**6,
                transcendentals=0,
            ),
        )(*operands)

    operand = jax.ShapeDtypeStruct((depth, lanes), dtype)
    right_first, right_next = call(
        early_kernel, (rows[0], rows[2]), (operand, operand), [], 0, 8
    )
    paths = call(
        begin_kernel,
        (own, right_first),
        jax.ShapeDtypeStruct((depth, lanes), jnp.float32),
        [left],
        len(FIRST),
        16,
    )
    payload = call(
        count_kernel,
        (own, oth, *rows[1:], right_next, paths),
        jax.ShapeDtypeStruct((64, 8, 128), jnp.float32),
        [left, left, right, right, acc],
        len(REST),
        24,
    )
    peers = [
        [(2 * chip + core) * 8 + c for chip in range(8) for c in range(8)]
        for core in range(2)
    ]
    parts = lax.all_to_all(payload, ALL, 0, 0, axis_index_groups=peers, tiled=True)
    across = lax.ppermute(parts, "row", [(r, r ^ 1) for r in range(16)])
    clustering, transitivity = pl.pallas_call(
        finish_kernel,
        out_shape=(
            jax.ShapeDtypeStruct((1, 80), jnp.float32),
            jax.ShapeDtypeStruct((1, 1), jnp.float32),
        ),
        in_specs=[vmem] * 3,
        out_specs=(vmem, vmem),
        compiler_params=pltpu.CompilerParams(vmem_limit_bytes=4 * 2**20),
        name="finish",
    )(parts, across, relabel[None])
    return clustering[0], transitivity[0, 0]


def solution(mesh):
    return jax.shard_map(
        body,
        mesh=mesh,
        in_specs=(P("row", "col"), P(ALL)),
        out_specs=(P(ALL), P()),
        check_vma=False,
    )
```

```python
import jax
import jax.numpy as jnp
from jax import lax
from jax.experimental import pallas as pl
from jax.experimental.pallas import tpu as pltpu
from jax.sharding import PartitionSpec as P

ALL = ("row", "col")
WINDOW = 5


def spread(value, peers):
    return jnp.broadcast_to(value[None], (peers, *value.shape))


def shifted(row, step):
    words = jnp.broadcast_to(row, (32, row.shape[1]))
    return lax.shift_right_logical(words, step)


def weighted(row, weight, dtype):
    bit = lax.broadcasted_iota(jnp.int32, (32, row.shape[1]), 0)
    value = (shifted(row, bit).astype(jnp.int8) & jnp.int8(1)).astype(jnp.bfloat16)
    return (value * weight if weight != 1 else value).astype(dtype)


FIRST = (((0, 0), (0, 2)),)
REST = (((1, 0), (1, 2)), ((0, 4), (1, 4)), ((0, 1), (1, 1)), ((0, 3), (1, 3)))
WEIGHTS = (1, 2, 2, 2, 1)
PART = 384


TILE = 256


def fill_right(target, rows, step, tile, core):
    half = 20
    for w in range(8 * tile, 8 * tile + 8):
        side, t = step[w // half]
        base = half * (core if side == 0 else 1 - core) + w % half
        row = rows[t][pl.ds(base, 1), :]
        target[w * 32 : w * 32 + 32, : row.shape[1]] = weighted(
            row, WEIGHTS[t], target.dtype
        )


def fill_left(target, sources, step, tile, places):
    for k, (side, t) in enumerate(step):
        words = sources[side][places[t], 8 * tile : 8 * tile + 8, :]
        octets = jnp.concatenate(
            [lax.shift_right_logical(words, jnp.int32(8 * byte)) for byte in range(4)], axis=0
        ).astype(jnp.int8)
        for s in range(8):
            picked = octets & jnp.int8(-128 if s == 7 else 1 << s)
            at = tile * TILE + s * 32
            target[at : at + 32, k * 640 : k * 640 + 640] = picked.astype(
                jnp.bfloat16
            ).astype(target.dtype)


def label_of(col):
    return (col % 4) * 2 + col // 4


def place_of(label):
    return (label % 2) * 4 + (label % 8) // 2


def places_of(col):
    return [place_of(label_of(col) + t) for t in range(WINDOW)]


def early_kernel(r0, r2, right_first, right_next):
    core = lax.rem(lax.axis_index("row"), 2)
    rows = (r0, None, r2)
    for tile in range(5):
        fill_right(right_first, rows, FIRST[0], tile, core)
        fill_right(right_next, rows, REST[0], tile, core)


def product(left, right, first, count, lanes=640):
    return jnp.dot(
        left[first : first + count, :],
        right[:, :lanes],
        preferred_element_type=jnp.float32,
    )


def masked_sum(total, value, first, words_of):
    for chunk in range(first // 32, (first + value.shape[0]) // 32):
        tile, s = chunk // 8, chunk % 8
        words = words_of(tile)
        part = 0.0
        for byte in range(4):
            at = chunk * 32 - first + byte * 8
            spot = 8 * byte + s
            hit = (words & jnp.int32(-(2**31) if spot == 31 else 1 << spot)) != 0
            part = part + jnp.where(hit, value[at : at + 8, :], 0.0)
        total = total + part * (-(2.0**-7) if s == 7 else 2.0**-s)
    return total


def begin_kernel(own, right, paths, left):
    places = places_of(lax.axis_index("col"))
    filled = 0
    for first in range(0, 1280, 640):
        while filled < 5 and filled * TILE < first + 2 * 640:
            fill_left(left, (own,), FIRST[0], filled, places)
            filled += 1
        paths[first : first + 640, :] = product(left, right, first, 640)


def count_kernel(own, oth, r1, r2, r3, r4, right_next, paths, out, la, lb, ra, rb, acc):
    chip = lax.axis_index("row") // 2
    core = lax.rem(lax.axis_index("row"), 2)
    col = lax.axis_index("col")
    places = places_of(col)
    mask = own.at[chip]
    rows = (mask, r1, r2, r3, r4)
    lanes = r1.shape[1]
    left, right = (la, lb), (ra, rb)
    for tile in range(5):
        fill_left(la, (own, oth), REST[0], tile, places)
    low = label_of(col) < 4
    part_lane = lax.broadcasted_iota(jnp.int32, (8, PART), 1)

    def all_words(tile):
        return mask[8 * tile : 8 * tile + 8, :]

    def part_words(tile):
        words = all_words(tile)
        picked = jnp.where(low, words[:, :PART], words[:, lanes - PART :])
        return jnp.where(low | (part_lane >= 2 * PART - lanes), picked, 0)

    total = jnp.zeros((8, lanes), jnp.float32)
    shared = jnp.zeros((8, PART), jnp.float32)
    size = 640
    for k, step in enumerate(REST):
        now, later = k % 2, (k + 1) % 2
        known = paths if k == 0 else acc
        factor = right_next if k == 0 else right[now]
        opposite = step[0][1] == 4
        filled = 0
        for first in range(0, 1280, size):
            while k + 1 < len(REST) and filled < 5 and filled * TILE < first + size:
                fill_left(left[later], (own, oth), REST[k + 1], filled, places)
                fill_right(right[later], rows, REST[k + 1], filled, core)
                filled += 1
            if opposite:
                value = product(left[now], factor, first, size, PART)
                shared = masked_sum(shared, value, first, part_words)
                continue
            value = known[first : first + size, :] + product(left[now], factor, first, size)
            if k + 1 < len(REST):
                acc[first : first + size, :] = value
            else:
                total = masked_sum(total, value, first, all_words)
    closed = jnp.sum(total, axis=0, keepdims=True)
    halves = 2.0 * jnp.sum(shared, axis=0, keepdims=True)
    above = jnp.zeros((1, lanes - PART), jnp.float32)
    closed = closed + jnp.where(
        low,
        jnp.concatenate([halves, above], axis=1),
        jnp.concatenate([above, halves], axis=1),
    )
    links = sum(lax.population_count(rows[t][...]) for t in range(4))
    degree = jnp.sum(links, axis=0, keepdims=True).astype(jnp.float32)
    part = label_of(col) % 4
    first = jnp.where(
        part == 0,
        degree[:, :128],
        jnp.where(part == 1, degree[:, 256:384], degree[:, 512:]),
    )
    second = jnp.where(part == 0, degree[:, 128:256], degree[:, 384:512])
    payload = jnp.concatenate(
        [closed[:, 128 * j : 128 * j + 128] for j in range(5)] + [first, second, first],
        axis=0,
    )
    out[...] = jnp.broadcast_to(payload[None], out.shape)


def reduced(parts):
    value = parts[...].reshape(8, 8, 8, 128)
    closed = value[:, :, :5].sum(axis=1)
    slots = [value[:, place_of(m), 5:7] + value[:, place_of(m + 4), 5:7] for m in range(3)]
    return closed, jnp.concatenate([slots[0], slots[1], slots[2][:, :1]], axis=1)


def interleaved(mine, other, core):
    first = jnp.where(core == 0, mine, other)
    second = jnp.where(core == 0, other, mine)
    return jnp.stack([first, second], axis=1).reshape(16, 5, 128)


def finish_kernel(own, oth, relabel, clustering, transitivity):
    core = lax.rem(lax.axis_index("row"), 2)
    closed, degree = (
        interleaved(mine, other, core) for mine, other in zip(reduced(own), reduced(oth))
    )
    wedges = jnp.maximum(degree * (degree - 1.0), 1.0)
    ratio = (closed / wedges).reshape(80, 128)
    index = relabel[...]
    line = index // 128
    lane = index - line * 128
    hot = (lax.broadcasted_iota(jnp.int32, (128, 80), 0) == lane).astype(jnp.float32)
    picked = jnp.dot(
        ratio, hot, preferred_element_type=jnp.float32, precision=lax.Precision.HIGHEST
    )
    mine = lax.broadcasted_iota(jnp.int32, (80, 80), 0) == line
    clustering[...] = jnp.sum(jnp.where(mine, picked, 0.0), axis=0, keepdims=True)
    total = jnp.sum(closed.reshape(80, 128), axis=0, keepdims=True)
    pairs = jnp.sum(wedges.reshape(80, 128), axis=0, keepdims=True)
    transitivity[...] = jnp.sum(total, axis=1, keepdims=True) / jnp.sum(
        pairs, axis=1, keepdims=True
    )


def body(adjacency, relabel, dtype=jnp.float8_e4m3fn):
    words = adjacency.T
    cores = [[2 * chip + core for chip in range(8)] for core in range(2)]
    own = lax.all_to_all(
        spread(words, 8), "row", 0, 0, axis_index_groups=cores, tiled=True
    )
    rows = [words]
    start = jnp.where(label_of(lax.axis_index("col")) < 4, words.shape[1] - PART, 0)
    opposite = lax.dynamic_slice_in_dim(words, start, PART, axis=1)
    for t in range(1, WINDOW):
        sent = words if t < 4 else opposite
        rows.append(
            lax.ppermute(
                sent, "col", [(place_of(label_of(c) + t), c) for c in range(8)]
            )
        )
    oth = lax.ppermute(own, "row", [(r, r ^ 1) for r in range(16)])
    vmem = pl.BlockSpec(memory_space=pltpu.VMEM)
    depth = words.shape[0] * 32
    lanes = words.shape[1]
    left = pltpu.VMEM((depth, depth), dtype)
    right = pltpu.VMEM((depth, lanes), dtype)
    acc = pltpu.VMEM((depth, lanes), jnp.float32)

    def call(kernel, operands, out_shape, scratch, steps, mib):
        return pl.pallas_call(
            kernel,
            out_shape=out_shape,
            in_specs=[vmem] * len(operands),
            out_specs=jax.tree.map(lambda _: vmem, out_shape),
            scratch_shapes=scratch,
            compiler_params=pltpu.CompilerParams(vmem_limit_bytes=mib * 2**20),
            cost_estimate=pl.CostEstimate(
                flops=max(2 * steps * depth * depth * lanes, 10**8),
                bytes_accessed=5 * 10**6,
                transcendentals=0,
            ),
        )(*operands)

    operand = jax.ShapeDtypeStruct((depth, lanes), dtype)
    right_first, right_next = call(
        early_kernel, (rows[0], rows[2]), (operand, operand), [], 0, 8
    )
    paths = call(
        begin_kernel,
        (own, right_first),
        jax.ShapeDtypeStruct((depth, lanes), jnp.float32),
        [left],
        len(FIRST),
        16,
    )
    payload = call(
        count_kernel,
        (own, oth, *rows[1:], right_next, paths),
        jax.ShapeDtypeStruct((64, 8, 128), jnp.float32),
        [left, left, right, right, acc],
        len(REST),
        24,
    )
    peers = [
        [(2 * chip + core) * 8 + c for chip in range(8) for c in range(8)]
        for core in range(2)
    ]
    parts = lax.all_to_all(payload, ALL, 0, 0, axis_index_groups=peers, tiled=True)
    across = lax.ppermute(parts, "row", [(r, r ^ 1) for r in range(16)])
    clustering, transitivity = pl.pallas_call(
        finish_kernel,
        out_shape=(
            jax.ShapeDtypeStruct((1, 80), jnp.float32),
            jax.ShapeDtypeStruct((1, 1), jnp.float32),
        ),
        in_specs=[vmem] * 3,
        out_specs=(vmem, vmem),
        compiler_params=pltpu.CompilerParams(vmem_limit_bytes=4 * 2**20),
        name="finish",
    )(parts, across, relabel[None])
    return clustering[0], transitivity[0, 0]


def solution(mesh):
    return jax.shard_map(
        body,
        mesh=mesh,
        in_specs=(P("row", "col"), P(ALL)),
        out_specs=(P(ALL), P()),
        check_vma=False,
    )
```
